32 devices in a mesh: dp: 8 (over y, x, core), mp: 4 (over z).
Axes of the slice: x: 2, y: 2, z: 4, core: 2. Of those that a mesh axis runs over, the one named last changes fastest.
Arguments:
- tokens: bfloat16 [2048, 6144], P('dp', 'mp'), may hold values from -40 to 40
- norm_gain: float32 [6144], P('mp'), may hold values from 0.1 to 1.9
- w_qkv: bfloat16 [6144, 3, 4096], P('mp', None, 'dp'), may hold values from -0.078125 to 0.078125
- w_up: bfloat16 [6144, 12288], P('mp', 'dp'), may hold values from -0.078125 to 0.078125
- w_attn_out: bfloat16 [4096, 6144], P('dp', 'mp'), may hold values from -0.09375 to 0.09375
- w_down: bfloat16 [12288, 6144], P('dp', 'mp'), may hold values from -0.0546875 to 0.0546875
Outputs:
- layer_out: bfloat16 [2048, 6144], P('dp', 'mp')
The draws below stay inside these ranges and needn't reach their ends.
All inputs are finite; a program needn't handle non-finite values.
Results may differ from the reference program's by a relative error of at most 0.015.
Values may be sent and summed in bfloat16 or wider, within the bound.
No kernel may reach another device: no remote copies, remote signals or barrier semaphores. Data moves between devices by JAX's collectives and lax.ppermute only.
A program may use at most 128 MiB of HBM per device.

```python
import jax
import jax.numpy as jnp
from jax import lax

D = 6144
HEADS = 32
HEAD_DIM = 128
FF = 12288
PATCHES = 256
TOKENS = 2048
N_DP = 8
N_MP = 4


def draw_tokens(key, part):
    first = jax.random.fold_in(key, 0)
    ramp = 0.6 * 3.0 ** (jnp.arange(D, dtype=jnp.float32) / D)
    values = jnp.clip(jax.random.normal(first, (TOKENS, D), jnp.float32), -6.0, 6.0) * ramp[None, :]
    return values.astype(jnp.bfloat16)


def levels(own_key, extent, pieces, low, largest):
    level = 1.0
    for dim, blocks in pieces:
        steps = jax.random.uniform(jax.random.fold_in(jax.random.fold_in(own_key, 6), dim), (blocks,), jnp.float32, low / len(pieces), largest / len(pieces))
        level = level * jnp.repeat(jnp.exp(steps), extent[dim] // blocks).reshape((-1,) + (1,) * (len(extent) - 1 - dim))
    return level


def bell_draw(rng, dims, deviation, most, pieces=(), held_as=jnp.bfloat16):
    loudness = levels(rng, dims, pieces, -0.22, 0.18) if pieces else 1.0
    drawn = jax.random.normal(rng, dims, jnp.float32) * deviation * loudness
    return jnp.minimum(jnp.maximum(drawn, -most), most).astype(held_as)


def setup_inputs(seed: int = 0) -> dict:
    splits = jax.random.split(jax.random.key(seed), 7)
    return {
        "tokens": draw_tokens(jax.random.fold_in(splits[6], 71), 0),
        "norm_gain": jnp.clip(1.0 + 0.18 * jax.random.normal(splits[1], (D,), jnp.float32), 0.1, 1.9),
        "w_qkv": bell_draw(splits[2], (D, 3, HEADS * HEAD_DIM), D ** -0.5, 0.078125, ((0, 4), (2, 8))),
        "w_up": bell_draw(splits[3], (D, FF), D ** -0.5, 0.078125, ((0, 4), (1, 8))),
        "w_attn_out": bell_draw(splits[4], (HEADS * HEAD_DIM, D), (HEADS * HEAD_DIM) ** -0.5, 0.09375, ((0, 8), (1, 4))),
        "w_down": bell_draw(splits[5], (FF, D), FF ** -0.5, 0.0546875, ((0, 8), (1, 4))),
    }


EPS = 1e-06

def normalize_rows(values, total, squares, gain, width):
    mean = total / width
    spread = squares / width - mean * mean
    scaled = (values - mean[:, None]) * lax.rsqrt(spread + EPS)[:, None]
    return (scaled * gain[None, :]).astype(jnp.bfloat16)

def head_norm(values):
    mean = lax.optimization_barrier(jnp.mean(values, axis=-1, keepdims=True))
    centered = values - mean
    spread = lax.optimization_barrier(jnp.mean(centered * centered, axis=-1, keepdims=True))
    return centered * lax.rsqrt(spread + EPS)

def attend(qkv, heads_here):
    rows = qkv.shape[0]
    images = rows // PATCHES
    parts = qkv.reshape(images, PATCHES, 3, heads_here, HEAD_DIM)
    query = (head_norm(parts[:, :, 0].astype(jnp.float32)) * (1.0 / HEAD_DIM) ** 0.5).astype(jnp.bfloat16)
    keys = head_norm(parts[:, :, 1].astype(jnp.float32)).astype(jnp.bfloat16)
    values = parts[:, :, 2]
    scores = jnp.einsum('iqhd,ikhd->ihqk', query.astype(jnp.float32), keys.astype(jnp.float32))
    weights = jnp.exp(scores)
    probs = (weights / lax.optimization_barrier(jnp.sum(weights, axis=-1, keepdims=True))).astype(jnp.bfloat16)
    mixed = jnp.einsum('ihqk,ikhd->iqhd', probs.astype(jnp.float32), values.astype(jnp.float32))
    return mixed.astype(jnp.bfloat16).reshape(rows, heads_here * HEAD_DIM)

def reference(tokens, norm_gain, w_qkv, w_up, w_attn_out, w_down):
    xf = tokens.astype(jnp.float32)
    normed = normalize_rows(xf, lax.optimization_barrier(jnp.sum(xf, axis=1)), lax.optimization_barrier(jnp.sum(xf * xf, axis=1)), norm_gain, D)
    head_cols = HEADS * HEAD_DIM
    w_heads = w_qkv.reshape(D, 3 * head_cols)
    feat_block = D // N_MP
    projected = jnp.zeros((TOKENS, 3 * head_cols + FF), jnp.float32)
    for block in range(N_MP):
        first = block * feat_block
        cols = normed[:, first:first + feat_block]
        term = jnp.concatenate([jnp.dot(cols, w_heads[first:first + feat_block], preferred_element_type=jnp.float32), jnp.dot(cols, w_up[first:first + feat_block], preferred_element_type=jnp.float32)], axis=1)
        projected = projected + lax.optimization_barrier(term.astype(jnp.bfloat16)).astype(jnp.float32)
    projected = projected.astype(jnp.bfloat16)
    qkv = projected[:, :3 * head_cols].reshape(TOKENS, 3, head_cols)
    attended = attend(qkv, HEADS)
    activated = jax.nn.gelu(projected[:, 3 * head_cols:].astype(jnp.float32)).astype(jnp.bfloat16)
    head_block = head_cols // N_DP
    unit_block = FF // N_DP
    total = xf
    for block in range(N_DP):
        hfirst = block * head_block
        ufirst = block * unit_block
        term = jnp.dot(attended[:, hfirst:hfirst + head_block], w_attn_out[hfirst:hfirst + head_block], preferred_element_type=jnp.float32)
        term = term + jnp.dot(activated[:, ufirst:ufirst + unit_block], w_down[ufirst:ufirst + unit_block], preferred_element_type=jnp.float32)
        total = total + lax.optimization_barrier(term.astype(jnp.bfloat16)).astype(jnp.float32)
    return total.astype(jnp.bfloat16)
```

```python
import functools
import itertools

import jax
import jax.numpy as jnp
from jax import lax
from jax.experimental import pallas as pl
from jax.sharding import PartitionSpec as P


HEAD_DIM = 128
PATCHES = 256
GROUPS = 4
HOP_IN = 2
HOP_OUT = 2
GATHER = 2

EPS = 1e-06


def head_norm(values):
    mean = jnp.mean(values, axis=-1, keepdims=True)
    centered = values - mean
    spread = jnp.mean(centered * centered, axis=-1, keepdims=True)
    return centered * lax.rsqrt(spread + EPS)


def block_kernel(*refs, heads_here, head_cols, groups):
    ins, outs = refs[:groups], refs[groups:]
    piece = ins[0].shape[1]
    for s, h in itertools.product(range(2), range(heads_here)):
        first = h * HEAD_DIM
        query, keys, values = (
            jnp.concatenate(
                [r[s, :, k * head_cols + first : k * head_cols + first + HEAD_DIM] for r in ins],
                axis=0,
            )
            for k in range(3)
        )
        query = (head_norm(query.astype(jnp.float32)) * (1.0 / HEAD_DIM) ** 0.5).astype(jnp.bfloat16)
        keys = head_norm(keys.astype(jnp.float32)).astype(jnp.bfloat16)
        scores = lax.dot_general(
            query, keys, (((1,), (1,)), ((), ())), preferred_element_type=jnp.float32
        )
        weights = jnp.exp(scores)
        probs = (weights / jnp.sum(weights, axis=-1, keepdims=True)).astype(jnp.bfloat16)
        mixed = jnp.dot(probs, values, preferred_element_type=jnp.float32).astype(jnp.bfloat16)
        for g in range(groups):
            outs[g][s, :, first : first + HEAD_DIM] = mixed[g * piece : (g + 1) * piece]
    for g in range(groups):
        up = ins[g][:, :, 3 * head_cols :].astype(jnp.float32)
        outs[g][:, :, head_cols:] = jax.nn.gelu(up).astype(jnp.bfloat16)


def block(chunks, heads_here, head_cols):
    sets, rows, cols = chunks[0].shape
    return pl.pallas_call(
        functools.partial(
            block_kernel, heads_here=heads_here, head_cols=head_cols, groups=len(chunks)
        ),
        out_shape=[jax.ShapeDtypeStruct((sets, rows, cols - 2 * head_cols), jnp.bfloat16)] * len(chunks),
    )(*chunks)


def dp_bits(n_dp):
    bits = []
    bit = n_dp // 2
    while bit > 1:
        bits.append(bit)
        bit //= 2
    return bits


def swap(values, bit, n_dp):
    return lax.ppermute(values, "dp", [(i, i ^ bit) for i in range(n_dp)])


def scatter_dp(blocks, order, n_dp, me):
    live = dict(enumerate(blocks))
    for bit in order:
        low = [d for d in live if d & bit == 0]
        is_low = (me & bit) == 0
        first = jnp.stack([live[d] for d in low])
        second = jnp.stack([live[d | bit] for d in low])
        got = swap(jnp.where(is_low, second, first), bit, n_dp)
        kept = jnp.where(is_low, first, second)
        total = (kept.astype(jnp.float32) + got.astype(jnp.float32)).astype(jnp.bfloat16)
        live = {d: total[k] for k, d in enumerate(low)}
    return live[0]


def pick(position, choices):
    out = choices[0]
    for k in range(1, len(choices)):
        out = jnp.where(position == k, choices[k], out)
    return out


def local(tokens, norm_gain, w_qkv, w_up, w_attn_out, w_down):
    n_mp = lax.axis_size("mp")
    n_dp = lax.axis_size("dp")
    z = lax.axis_index("mp")
    me = lax.axis_index("dp")
    rows_here, feat_here = tokens.shape
    head_cols = w_qkv.shape[2]
    heads_here = head_cols // HEAD_DIM
    width = feat_here * n_mp
    own_images = rows_here // PATCHES
    images = own_images * n_dp
    half = images // 2
    piece = PATCHES // GROUPS
    core = me % 2
    half_cols = feat_here // 2
    bits = dp_bits(n_dp)
    order, order_b = [1] + bits, [1] + bits[::-1]

    def swap_cores(values):
        return lax.ppermute(values, "dp", [(i, i ^ 1) for i in range(n_dp)])

    def along(values, hops, way):
        pairs = []
        for d in range(n_dp):
            for p in hops:
                up = (d % 2 == 1) == (way > 0)
                source, target = (p, p + 1) if up else (n_mp - 1 - p, n_mp - 2 - p)
                pairs.append((d * n_mp + source, d * n_mp + target))
        return lax.ppermute(values, ("dp", "mp"), pairs)

    tokens_f = tokens.astype(jnp.float32)
    total, squares = lax.psum(
        (jnp.sum(tokens_f, axis=1), jnp.sum(tokens_f * tokens_f, axis=1)), "mp"
    )
    mean = total / width
    spread = squares / width - mean * mean
    normed = ((tokens_f - mean[:, None]) * lax.rsqrt(spread + EPS)[:, None] * norm_gain[None, :]).astype(jnp.bfloat16)
    normed = normed.reshape(own_images, PATCHES, feat_here)

    w_in = jnp.concatenate([w_qkv.reshape(feat_here, 3 * head_cols), w_up], axis=1)

    partial = []
    for g in range(GROUPS):
        if g % GATHER == 0:
            rows = normed[:, g * piece : (g + GATHER) * piece]
            wide = lax.all_gather(rows, "dp", axis=0, tiled=True)
        every = wide[:, g % GATHER * piece : (g % GATHER + 1) * piece]
        every = every.reshape(images * piece, feat_here)
        if g:
            every, _ = lax.optimization_barrier((every, partial[g - 2] if g > 1 else sent))
        term = jnp.dot(every, w_in, preferred_element_type=jnp.float32).astype(jnp.bfloat16)
        term = term.reshape(2, half, piece, -1)
        kept = jnp.where(core == 0, term[0], term[1])
        sent = jnp.where(core == 0, term[1], term[0])
        other = swap_cores(sent)
        partial.append(jnp.stack([kept, other], axis=1))

    count = GROUPS * half
    spans = [(c // half, c % half) for c in range(count)]

    def chunk(c):
        g, i = spans[min(max(c, 0), count - 1)]
        return partial[g][i]

    position = jnp.where(core == 0, n_mp - 1 - z, z)
    got = {}
    final = []
    last = HOP_IN * (n_mp - 1)
    for t in range(count + last):
        reach = min(n_mp, t // HOP_IN + 1)
        sums = pick(position, [chunk(t - HOP_IN * p) for p in range(reach)])
        if t >= HOP_IN:
            came, _ = lax.optimization_barrier((got[t - HOP_IN], before))
            sums = sums.astype(jnp.float32) + came.astype(jnp.float32)
            sums = sums.astype(jnp.bfloat16)
        before = sums
        if t >= last:
            final.append(sums)
        if t < count + last - HOP_IN:
            hops = [p for p in range(n_mp - 1) if 0 <= t - HOP_IN * p < count]
            got[t] = along(sums, hops, 1)

    own = [None] * count
    for i in range(half):
        made = block([final[g * half + i] for g in range(GROUPS)], heads_here, head_cols)
        for g in range(GROUPS):
            own[g * half + i] = made[g]

    position = jnp.where(core == 0, z, n_mp - 1 - z)
    passed = []
    for t in range(count + HOP_OUT * (n_mp - 2)):
        mine = own[min(t, count - 1)]
        if t >= HOP_OUT:
            mine = jnp.where(position == 0, mine, passed[t - HOP_OUT])
        hops = [p for p in range(n_mp - 1) if 0 <= t - HOP_OUT * p < count]
        passed.append(along(mine, hops, -1))

    pieces = []
    for g in range(GROUPS):
        rows = []
        for i in range(half):
            c = g * half + i
            rows.append(
                pick(position, [own[c]] + [passed[c + HOP_OUT * (p - 1)] for p in range(1, n_mp)])
            )
        rows = jnp.stack(rows)
        kept = rows[:, 0]
        other = swap_cores(rows[:, 1])
        hidden = jnp.concatenate(
            [jnp.where(core == 0, kept, other), jnp.where(core == 0, other, kept)], axis=0
        ).reshape(images * piece, -1)
        result = jnp.dot(hidden[:, :head_cols], w_attn_out, preferred_element_type=jnp.float32)
        result = result + jnp.dot(hidden[:, head_cols:], w_down, preferred_element_type=jnp.float32)
        result = result.astype(jnp.bfloat16).reshape(n_dp, own_images, piece, feat_here)
        left = scatter_dp([result[d, ..., :half_cols] for d in range(n_dp)], order, n_dp, me)
        right = scatter_dp([result[d, ..., half_cols:] for d in range(n_dp)], order_b, n_dp, me)
        pieces.append(jnp.concatenate([left, right], axis=-1))
    summed = jnp.concatenate(pieces, axis=1).reshape(rows_here, feat_here).astype(jnp.float32)
    return (tokens_f + summed).astype(jnp.bfloat16)


def solution(mesh):
    placed = (
        P("dp", "mp"),
        P("mp"),
        P("mp", None, "dp"),
        P("mp", "dp"),
        P("dp", "mp"),
        P("dp", "mp"),
    )

    return jax.shard_map(
        local, mesh=mesh, in_specs=placed, out_specs=P("dp", "mp"), check_vma=False
    )
```
